32 devices in a mesh: dp: 8 (over z, x), tensor: 4 (over y, core).
Axes of the slice: x: 2, y: 2, z: 4, core: 2. Of those that a mesh axis runs over, the one named last changes fastest.
Arguments:
- activations: bfloat16 [16, 128, 4096], P('dp'), may hold values from -6 to 6
- out_grads: bfloat16 [16, 128, 20480], P('dp', None, 'tensor'), may hold values from -0.875 to 0.875
- act_scale: bfloat16 [16, 32], P('dp'), may hold values from 1 to 16
- grad_scale: bfloat16 [16, 1, 20480], P('dp', None, 'tensor'), may hold values from 1 to 72
- moment: float32 [20480, 4096], P(('tensor', 'dp')), may hold values from -0.6 to 0.6
- second: float32 [20480, 4096], P(('tensor', 'dp')), may hold values from 0.1 to 1
- master: float32 [20480, 4096], P(('tensor', 'dp')), may hold values from -0.0625 to 0.0625
Outputs:
- new_moment: float32 [20480, 4096], P(('tensor', 'dp'))
- new_second: float32 [20480, 4096], P(('tensor', 'dp'))
- new_master: float32 [20480, 4096], P(('tensor', 'dp'))
- weights: bfloat16 [20480, 4096], P(('tensor', 'dp'))
The draws below stay inside these ranges and needn't reach their ends.
All inputs are finite; a program needn't handle non-finite values.
Results may differ from the reference program's by a relative error of at most 0.015.
Values may be sent and summed in bfloat16 or wider, within the bound.
A program may use at most 192 MiB of HBM per device.

```python
import math
import jax
import jax.numpy as jnp
from jax import lax

FF = 20480
ROWS = 4096
TILE = 128
TOK_DEV = 256
TOKENS = 2048
BLOCKS = 16
N_DP = 8


def draw_act_scale(key, part):
    upper = math.log(10.0)
    values = jnp.exp(jax.random.uniform(key, (BLOCKS, ROWS // TILE), jnp.float32, 0.0, upper))
    return values.astype(jnp.bfloat16)


def draw_grad_scale(key, part):
    upper = math.log(4.0)
    columns = jnp.arange(FF, dtype=jnp.float32) / (FF - 1)
    riser = jnp.exp(columns * math.log(9.0))
    base = jnp.exp(jax.random.uniform(key, (BLOCKS, 1, FF), jnp.float32, 0.0, upper))
    return (base * riser[None, None, :]).astype(jnp.bfloat16)


def with_spikes(values, rng, source, target, parts, factor):
    owner, partner = [(jnp.arange(values.shape[axis_at]) // (values.shape[axis_at] // parts)).reshape([-1 if axis == axis_at else 1 for axis in range(values.ndim)]) for axis_at in (source, target)]
    chosen = jax.random.permutation(rng, parts)[partner]
    strong = (owner == chosen) | (owner == (partner + parts // 2) % parts)
    return jnp.where(strong, factor * values, values)


def steps_of(key, extent, split, least, largest):
    gain, own = 1.0, jax.random.fold_in(key, 6)
    for dim, blocks in split:
        draws = jnp.exp(jax.random.uniform(jax.random.fold_in(own, dim), (blocks,), jnp.float32, least / len(split), largest / len(split)))
        gain = gain * jnp.repeat(draws, extent[dim] // blocks).reshape([-1 if axis == dim else 1 for axis in range(len(extent))])
    return gain


def scatter_about(rng, extent, scale, most, pieces=(), held_as=jnp.bfloat16):
    level = steps_of(rng, extent, pieces, -0.22, 0.18) if pieces else 1.0
    drawn = jax.random.normal(rng, extent, jnp.float32) * scale * level
    return jnp.minimum(jnp.maximum(drawn, -most), most).astype(held_as)


def gaussian_with(key, shape, deviation, reach, pieces, heavy, kind=jnp.bfloat16):
    entries = deviation * jax.random.normal(key, shape, jnp.float32)
    if pieces:
        entries = entries * steps_of(key, shape, pieces, -0.22, 0.18)
    return jnp.clip(with_spikes(entries, jax.random.fold_in(key, 3), *heavy), -reach, reach).astype(kind)


def setup_inputs(seed: int = 0) -> dict:
    streams_of = jax.random.split(jax.random.key(seed), 8)
    activations = scatter_about(streams_of[0], (BLOCKS, TILE, ROWS), 1.0, 6.0, ((0, 8),))
    out_grads = gaussian_with(streams_of[1], (BLOCKS, TILE, FF), (2.0 / TOKENS ** 0.5), 0.875, ((0, 8), (2, 4)), (0, 2, 8, 2.0))
    act_scale = draw_act_scale(jax.random.fold_in(streams_of[7], 71), 0)
    grad_scale = draw_grad_scale(jax.random.fold_in(streams_of[7], 71), 0)
    moment = scatter_about(streams_of[4], (FF, ROWS), 0.1, 0.6, ((0, 32),), jnp.float32)
    second = jnp.clip(jnp.exp(math.log(1.0) - 2.3025851 * jax.random.uniform(streams_of[5], (FF, ROWS), jnp.float32) ** steps_of(streams_of[5], (FF, ROWS), ((0, 32),), -0.2, 0.2)), 0.1, 1.0)
    master = scatter_about(streams_of[6], (FF, ROWS), 8192 ** -0.5, 0.0625, ((0, 32),), jnp.float32)
    return dict(activations=activations, out_grads=out_grads, act_scale=act_scale, grad_scale=grad_scale, moment=moment, second=second, master=master)


clip_rms = 1.0
beta_first = 0.9
beta_second = 0.95
learn_rate = 0.003
adam_eps = 1e-08

def widen(act_scale):
    tiles = act_scale.astype(jnp.float32)
    spread = jnp.broadcast_to(tiles[:, :, None], tiles.shape + (TILE,))
    return spread.reshape(tiles.shape[0], tiles.shape[1] * TILE)

def reference(activations, out_grads, act_scale, grad_scale, moment, second, master):
    acts_deq = (activations.astype(jnp.float32) * widen(act_scale)[:, None, :]).astype(jnp.bfloat16).reshape(TOKENS, ROWS)
    grads_deq = (out_grads.astype(jnp.float32) * grad_scale.astype(jnp.float32)).astype(jnp.bfloat16).reshape(TOKENS, FF)

    def add_group(group, total):
        start = (group * TOK_DEV).astype(jnp.int32)
        grads_group = lax.dynamic_slice_in_dim(grads_deq, start, TOK_DEV, 0)
        acts_group = lax.dynamic_slice_in_dim(acts_deq, start, TOK_DEV, 0)
        term = jnp.dot(grads_group.T, acts_group, preferred_element_type=jnp.float32)
        rounded = lax.optimization_barrier(term.astype(jnp.bfloat16))
        return total + rounded.astype(jnp.float32)
    grad = lax.fori_loop(0, N_DP, add_group, jnp.zeros((FF, ROWS), jnp.float32))
    norm = jnp.sqrt(jnp.sum(grad * grad))
    factor = jnp.minimum(1.0, clip_rms * jnp.sqrt(jnp.float32(FF * ROWS)) / norm)
    clipped = factor * grad
    new_moment = beta_first * moment + (1.0 - beta_first) * clipped
    new_second = beta_second * second + (1.0 - beta_second) * clipped * clipped
    new_master = master - learn_rate * new_moment / (jnp.sqrt(new_second) + adam_eps)
    weights = new_master.astype(jnp.bfloat16)
    return (new_moment, new_second, new_master, weights)
```

```python
import functools
import math

import jax
import jax.numpy as jnp
from jax import lax
from jax.experimental import pallas as pl
from jax.experimental.pallas import tpu as pltpu
from jax.sharding import PartitionSpec as P

MESH = pl.DeviceIdType.MESH
PAIR = 2

clip_rms = 1.0
beta_first = 0.9
beta_second = 0.95
learn_rate = 0.003
adam_eps = 1e-08


def gather_kernel(
    owners, lanes, acts, grads, full, moved, z_sem, x_sem, y_sem, c_sem, f_sem,
    g_send, own_sem, a_recv, g_recv,
):
    chain = owners // PAIR
    d = lax.axis_index("dp")
    t = lax.axis_index("tensor")
    g, b = d // PAIR, d % PAIR
    y, c = t // PAIR, t % PAIR
    x_dev = (g * PAIR + (1 - b), t)
    y_dev = (d, (1 - y) * PAIR + c)
    c_dev = (d, y * PAIR + (1 - c))
    across = (1 - y) * PAIR + c

    barrier = pltpu.get_barrier_semaphore()
    for o in range(1, owners):
        peer = (lax.rem(d + o, owners), t)
        pl.semaphore_signal(barrier, inc=1, device_id=peer, device_id_type=MESH)
    for peer in (y_dev, c_dev):
        pl.semaphore_signal(barrier, inc=1, device_id=peer, device_id_type=MESH)
    pl.semaphore_wait(barrier, owners + 1)

    def copy(src, slot, send, dev):
        return pltpu.make_async_remote_copy(
            src_ref=src, dst_ref=full.at[slot], send_sem=send, recv_sem=a_recv.at[slot],
            device_id=dev, device_id_type=MESH,
        )

    def held(s, q):
        return full.at[q * owners + s]

    def z_copy(s, up, src):
        to = g + 1 if up else g - 1
        return copy(src, t * owners + s, z_sem.at[up, s], (to * PAIR + b, t))

    def x_copy(s, src):
        return copy(src, t * owners + s, x_sem.at[s], x_dev)

    def y_copy(s):
        return copy(held(s, t), t * owners + s, y_sem.at[s], y_dev)

    def c_copy(s):
        return copy(held(s, t), t * owners + s, c_sem.at[s], c_dev)

    def f_copy(s):
        return copy(held(s, across), across * owners + s, f_sem.at[s], c_dev)

    def got(s, q):
        ref = held(s, q)
        pltpu.make_async_copy(ref, ref, a_recv.at[q * owners + s]).wait()

    def g_copy(o):
        to = lax.rem(d + o, owners)
        return pltpu.make_async_remote_copy(
            src_ref=grads.at[to], dst_ref=moved.at[d], send_sem=g_send.at[o],
            recv_sem=g_recv.at[d], device_id=(to, t), device_id_type=MESH,
        )

    mine = acts.at[t]

    @pl.when(g + 1 < chain)
    def _():
        z_copy(d, 1, mine).start()

    @pl.when(g > 0)
    def _():
        z_copy(d, 0, mine).start()

    x_copy(d, mine).start()
    own = [pltpu.make_async_copy(acts.at[q], held(d, q), own_sem.at[q]) for q in range(lanes)]
    own.append(pltpu.make_async_copy(grads.at[d], moved.at[d], own_sem.at[lanes]))
    for one in own:
        one.start()

    def below(k, act):
        pl.when(g - k >= 0)(lambda: act(g - k, 1))

    def above(k, act):
        pl.when(g + k < chain)(lambda: act(g + k, 0))

    def from_chain(at, up):
        s = at * PAIR + b
        got(s, t)
        onward = (g + 1 < chain) if up else (g > 0)
        pl.when(onward)(lambda: z_copy(s, up, held(s, t)).start())
        x_copy(s, held(s, t)).start()
        y_copy(s).start()
        c_copy(s).start()

    def from_pair(at, up):
        s = at * PAIR + (1 - b)
        got(s, t)
        y_copy(s).start()
        c_copy(s).start()

    def across_chain(at, up):
        s = at * PAIR + b
        got(s, across)
        f_copy(s).start()

    def across_pair(at, up):
        s = at * PAIR + (1 - b)
        got(s, across)
        f_copy(s).start()

    def ends(k, act):
        below(k, act)
        if k > 0:
            above(k, act)

    order = sorted(range(1, owners), key=lambda o: (abs(o - owners // 2), o))
    from_pair(g, 0)
    for k in range(1, chain):
        ends(k, from_chain)
        if k == min(2, chain - 1):
            for o in order:
                g_copy(o).start()
        if k > 1:
            ends(k - 1, from_pair)
        if k == 2:
            across_pair(g, 0)
        if k > 2:
            ends(k - 2, across_chain)
            ends(k - 2, across_pair)
    if chain > 1:
        ends(chain - 1, from_pair)
    if chain <= 2:
        across_pair(g, 0)
    for k in range(max(1, chain - 2), chain):
        ends(k, across_chain)
        ends(k, across_pair)

    for one in own:
        one.wait()
    for o in order:
        s = lax.rem(d + owners - o, owners)
        pltpu.make_async_copy(moved.at[s], moved.at[s], g_recv.at[s]).wait()
    beside = y * PAIR + (1 - c)
    corner = (1 - y) * PAIR + (1 - c)
    for o in range(1, owners):
        s = lax.rem(d + o, owners)
        got(s, beside)
        got(s, corner)

    for o in order:
        g_copy(o).wait_send()
    for o in range(1, owners):
        s = lax.rem(d + o, owners)
        y_copy(s).wait_send()
        c_copy(s).wait_send()
        f_copy(s).wait_send()
    x_copy(d, mine).wait_send()
    pl.when(g + 1 < chain)(lambda: z_copy(d, 1, mine).wait_send())
    pl.when(g > 0)(lambda: z_copy(d, 0, mine).wait_send())

    def chain_sent(at, up):
        s = at * PAIR + b
        onward = (g + 1 < chain) if up else (g > 0)
        pl.when(onward)(lambda: z_copy(s, up, held(s, t)).wait_send())
        x_copy(s, held(s, t)).wait_send()

    for k in range(1, chain):
        ends(k, chain_sent)


def gather_all(acts, grads, owners):
    lanes, tokens, quarter = acts.shape
    dma = pltpu.SemaphoreType.DMA
    return pl.pallas_call(
        functools.partial(gather_kernel, owners, lanes),
        out_shape=(
            jax.ShapeDtypeStruct((lanes * owners, tokens, quarter), acts.dtype),
            jax.ShapeDtypeStruct(grads.shape, grads.dtype),
        ),
        in_specs=[pl.BlockSpec(memory_space=pltpu.VMEM)] * 2,
        out_specs=(pl.BlockSpec(memory_space=pl.ANY),) * 2,
        scratch_shapes=[
            dma((2, owners)), dma((owners,)), dma((owners,)), dma((owners,)), dma((owners,)),
            dma((owners,)), dma((lanes + 1,)), dma((lanes * owners,)), dma((owners,)),
        ],
        compiler_params=pltpu.CompilerParams(collective_id=0, has_side_effects=True),
    )(acts, grads)


def norm_kernel(owners, lanes, limit, part, factor, near, far, own_sem, n_send, n_recv, f_send, f_recv):
    d = lax.axis_index("dp")
    t = lax.axis_index("tensor")
    barrier = pltpu.get_barrier_semaphore()
    for o in range(1, lanes):
        peer = (d, lax.rem(t + o, lanes))
        pl.semaphore_signal(barrier, inc=1, device_id=peer, device_id_type=MESH)
    for o in range(1, owners):
        peer = (lax.rem(d + o, owners), t)
        pl.semaphore_signal(barrier, inc=1, device_id=peer, device_id_type=MESH)
    pl.semaphore_wait(barrier, lanes + owners - 2)

    def near_copy(o):
        return pltpu.make_async_remote_copy(
            src_ref=part, dst_ref=near.at[t], send_sem=n_send.at[o], recv_sem=n_recv.at[t],
            device_id=(d, lax.rem(t + o, lanes)), device_id_type=MESH,
        )

    def far_copy(o):
        return pltpu.make_async_remote_copy(
            src_ref=near, dst_ref=far.at[d], send_sem=f_send.at[o], recv_sem=f_recv.at[d],
            device_id=(lax.rem(d + o, owners), t), device_id_type=MESH,
        )

    def got(ref, sem):
        pltpu.make_async_copy(ref, ref, sem).wait()

    for o in range(1, lanes):
        near_copy(o).start()
    own = pltpu.make_async_copy(part, near.at[t], own_sem)
    own.start()
    own.wait()
    for o in range(1, lanes):
        s = lax.rem(t + o, lanes)
        got(near.at[s], n_recv.at[s])
    for o in range(1, owners):
        far_copy(o).start()
    total = jnp.sum(near[...], axis=0)
    for o in range(1, owners):
        s = lax.rem(d + o, owners)
        got(far.at[s], f_recv.at[s])
        total += jnp.sum(far[s], axis=0)
    squares = jnp.sum(total, axis=(0, 1), keepdims=True)
    scale = jnp.minimum(1.0, limit / jnp.sqrt(squares))
    factor[...] = jnp.broadcast_to(scale, factor.shape)
    for o in range(1, lanes):
        near_copy(o).wait_send()
    for o in range(1, owners):
        far_copy(o).wait_send()


def clip_factor(part, owners, lanes, limit):
    dma = pltpu.SemaphoreType.DMA
    return pl.pallas_call(
        functools.partial(norm_kernel, owners, lanes, limit),
        out_shape=jax.ShapeDtypeStruct(part.shape, part.dtype),
        in_specs=[pl.BlockSpec(memory_space=pltpu.VMEM)],
        out_specs=pl.BlockSpec(memory_space=pltpu.VMEM),
        scratch_shapes=[
            pltpu.VMEM((lanes,) + part.shape, part.dtype),
            pltpu.VMEM((owners, lanes) + part.shape, part.dtype),
            dma, dma((lanes,)), dma((lanes,)), dma((owners,)), dma((owners,)),
        ],
        compiler_params=pltpu.CompilerParams(
            collective_id=1, has_side_effects=True, vmem_limit_bytes=4 * 1024 * 1024
        ),
    )(part)


def per_device(activations, out_grads, act_scale, grad_scale, moment, second, master):
    owners = lax.axis_size("dp")
    lanes = lax.axis_size("tensor")
    blocks, tile_tokens, weight_rows = activations.shape
    tiles = act_scale.shape[1]
    local_tokens = blocks * tile_tokens
    columns = out_grads.shape[2]
    owned = columns // owners
    entries = columns * lanes * weight_rows
    quarter = weight_rows // lanes
    spread = jnp.broadcast_to(
        act_scale.astype(jnp.float32)[:, :, None], (blocks, tiles, weight_rows // tiles)
    ).reshape(blocks, 1, weight_rows)
    acts_deq = (activations.astype(jnp.float32) * spread).astype(jnp.bfloat16)
    acts_deq = acts_deq.reshape(local_tokens, lanes, quarter).transpose(1, 0, 2)
    grads_deq = (out_grads.astype(jnp.float32) * grad_scale.astype(jnp.float32)).astype(jnp.bfloat16)
    grads_deq = grads_deq.reshape(local_tokens, owners, owned).transpose(1, 0, 2)
    piece, moved = gather_all(acts_deq, grads_deq, owners)
    total = owners * local_tokens
    moved = moved.reshape(total, owned)
    piece = piece.reshape(lanes, total, quarter)
    parts = []
    for t in range(lanes):
        parts.append(
            lax.dot_general(
                moved, piece[t], (((0,), (0,)), ((), ())), preferred_element_type=jnp.float32
            )
        )
    grad_owned = jnp.concatenate(parts, axis=1)
    part = jnp.sum((grad_owned * grad_owned).reshape(owned // 8, 8, weight_rows // 128, 128), axis=(0, 2))
    limit = clip_rms * math.sqrt(entries)
    factor = clip_factor(part, owners, lanes, limit)[0, 0]
    clipped = factor * grad_owned
    new_moment = beta_first * moment + (1.0 - beta_first) * clipped
    new_second = beta_second * second + (1.0 - beta_second) * clipped * clipped
    new_master = master - learn_rate * new_moment / (jnp.sqrt(new_second) + adam_eps)
    weights = new_master.astype(jnp.bfloat16)
    return (new_moment, new_second, new_master, weights)


def solution(mesh):
    return jax.shard_map(
        per_device,
        mesh=mesh,
        in_specs=(
            P("dp", None, None),
            P("dp", None, "tensor"),
            P("dp", None),
            P("dp", None, "tensor"),
            P(("tensor", "dp"), None),
            P(("tensor", "dp"), None),
            P(("tensor", "dp"), None),
        ),
        out_specs=(
            P(("tensor", "dp"), None),
            P(("tensor", "dp"), None),
            P(("tensor", "dp"), None),
            P(("tensor", "dp"), None),
        ),
        check_vma=False,
    )
```

```python
import functools
import math

import jax
import jax.numpy as jnp
from jax import lax
from jax.experimental import pallas as pl
from jax.experimental.pallas import tpu as pltpu
from jax.sharding import PartitionSpec as P

MESH = pl.DeviceIdType.MESH
PAIR = 2

clip_rms = 1.0
beta_first = 0.9
beta_second = 0.95
learn_rate = 0.003
adam_eps = 1e-08


def gather_kernel(
    owners, lanes, acts, grads, full, moved, z_sem, x_sem, y_sem, c_sem, f_sem,
    g_send, own_sem, a_recv, g_recv,
):
    chain = owners // PAIR
    d = lax.axis_index("dp")
    t = lax.axis_index("tensor")
    g, b = d // PAIR, d % PAIR
    y, c = t // PAIR, t % PAIR
    x_dev = (g * PAIR + (1 - b), t)
    y_dev = (d, (1 - y) * PAIR + c)
    c_dev = (d, y * PAIR + (1 - c))
    across = (1 - y) * PAIR + c

    barrier = pltpu.get_barrier_semaphore()
    for o in range(1, owners):
        peer = (lax.rem(d + o, owners), t)
        pl.semaphore_signal(barrier, inc=1, device_id=peer, device_id_type=MESH)
    for peer in (y_dev, c_dev):
        pl.semaphore_signal(barrier, inc=1, device_id=peer, device_id_type=MESH)
    pl.semaphore_wait(barrier, owners + 1)

    def copy(src, slot, send, dev):
        return pltpu.make_async_remote_copy(
            src_ref=src, dst_ref=full.at[slot], send_sem=send, recv_sem=a_recv.at[slot],
            device_id=dev, device_id_type=MESH,
        )

    def held(s, q):
        return full.at[q * owners + s]

    def z_copy(s, up, src):
        to = g + 1 if up else g - 1
        return copy(src, t * owners + s, z_sem.at[up, s], (to * PAIR + b, t))

    def x_copy(s, src):
        return copy(src, t * owners + s, x_sem.at[s], x_dev)

    def y_copy(s):
        return copy(held(s, t), t * owners + s, y_sem.at[s], y_dev)

    def c_copy(s):
        return copy(held(s, t), t * owners + s, c_sem.at[s], c_dev)

    def f_copy(s):
        return copy(held(s, across), across * owners + s, f_sem.at[s], c_dev)

    def got(s, q):
        ref = held(s, q)
        pltpu.make_async_copy(ref, ref, a_recv.at[q * owners + s]).wait()

    def g_copy(o):
        to = lax.rem(d + o, owners)
        return pltpu.make_async_remote_copy(
            src_ref=grads.at[to], dst_ref=moved.at[d], send_sem=g_send.at[o],
            recv_sem=g_recv.at[d], device_id=(to, t), device_id_type=MESH,
        )

    mine = acts.at[t]

    @pl.when(g + 1 < chain)
    def _():
        z_copy(d, 1, mine).start()

    @pl.when(g > 0)
    def _():
        z_copy(d, 0, mine).start()

    x_copy(d, mine).start()
    own = [pltpu.make_async_copy(acts.at[q], held(d, q), own_sem.at[q]) for q in range(lanes)]
    own.append(pltpu.make_async_copy(grads.at[d], moved.at[d], own_sem.at[lanes]))
    for one in own:
        one.start()

    def below(k, act):
        pl.when(g - k >= 0)(lambda: act(g - k, 1))

    def above(k, act):
        pl.when(g + k < chain)(lambda: act(g + k, 0))

    def from_chain(at, up):
        s = at * PAIR + b
        got(s, t)
        onward = (g + 1 < chain) if up else (g > 0)
        pl.when(onward)(lambda: z_copy(s, up, held(s, t)).start())
        x_copy(s, held(s, t)).start()
        y_copy(s).start()
        c_copy(s).start()

    def from_pair(at, up):
        s = at * PAIR + (1 - b)
        got(s, t)
        y_copy(s).start()
        c_copy(s).start()

    def across_chain(at, up):
        s = at * PAIR + b
        got(s, across)
        f_copy(s).start()

    def across_pair(at, up):
        s = at * PAIR + (1 - b)
        got(s, across)
        f_copy(s).start()

    def ends(k, act):
        below(k, act)
        if k > 0:
            above(k, act)

    order = sorted(range(1, owners), key=lambda o: (abs(o - owners // 2), o))
    from_pair(g, 0)
    for k in range(1, chain):
        ends(k, from_chain)
        if k == min(2, chain - 1):
            for o in order:
                g_copy(o).start()
        if k > 1:
            ends(k - 1, from_pair)
        if k == 2:
            across_pair(g, 0)
        if k > 2:
            ends(k - 2, across_chain)
            ends(k - 2, across_pair)
    if chain > 1:
        ends(chain - 1, from_pair)
    if chain <= 2:
        across_pair(g, 0)
    for k in range(max(1, chain - 2), chain):
        ends(k, across_chain)
        ends(k, across_pair)

    for one in own:
        one.wait()
    for o in order:
        s = lax.rem(d + owners - o, owners)
        pltpu.make_async_copy(moved.at[s], moved.at[s], g_recv.at[s]).wait()
    beside = y * PAIR + (1 - c)
    corner = (1 - y) * PAIR + (1 - c)
    for o in range(1, owners):
        s = lax.rem(d + o, owners)
        got(s, beside)
        got(s, corner)

    for o in order:
        g_copy(o).wait_send()
    for o in range(1, owners):
        s = lax.rem(d + o, owners)
        y_copy(s).wait_send()
        c_copy(s).wait_send()
        f_copy(s).wait_send()
    x_copy(d, mine).wait_send()
    pl.when(g + 1 < chain)(lambda: z_copy(d, 1, mine).wait_send())
    pl.when(g > 0)(lambda: z_copy(d, 0, mine).wait_send())

    def chain_sent(at, up):
        s = at * PAIR + b
        onward = (g + 1 < chain) if up else (g > 0)
        pl.when(onward)(lambda: z_copy(s, up, held(s, t)).wait_send())
        x_copy(s, held(s, t)).wait_send()

    for k in range(1, chain):
        ends(k, chain_sent)


def gather_all(acts, grads, owners):
    lanes, tokens, quarter = acts.shape
    dma = pltpu.SemaphoreType.DMA
    return pl.pallas_call(
        functools.partial(gather_kernel, owners, lanes),
        out_shape=(
            jax.ShapeDtypeStruct((lanes * owners, tokens, quarter), acts.dtype),
            jax.ShapeDtypeStruct(grads.shape, grads.dtype),
        ),
        in_specs=[pl.BlockSpec(memory_space=pltpu.VMEM)] * 2,
        out_specs=(pl.BlockSpec(memory_space=pl.ANY),) * 2,
        scratch_shapes=[
            dma((2, owners)), dma((owners,)), dma((owners,)), dma((owners,)), dma((owners,)),
            dma((owners,)), dma((lanes + 1,)), dma((lanes * owners,)), dma((owners,)),
        ],
        compiler_params=pltpu.CompilerParams(collective_id=0, has_side_effects=True),
    )(acts, grads)


def norm_kernel(owners, lanes, limit, part, factor, near, far, own_sem, n_send, n_recv, f_send, f_recv):
    d = lax.axis_index("dp")
    t = lax.axis_index("tensor")
    barrier = pltpu.get_barrier_semaphore()
    for o in range(1, lanes):
        peer = (d, lax.rem(t + o, lanes))
        pl.semaphore_signal(barrier, inc=1, device_id=peer, device_id_type=MESH)
    for o in range(1, owners):
        peer = (lax.rem(d + o, owners), t)
        pl.semaphore_signal(barrier, inc=1, device_id=peer, device_id_type=MESH)
    pl.semaphore_wait(barrier, lanes + owners - 2)

    def near_copy(o):
        return pltpu.make_async_remote_copy(
            src_ref=part, dst_ref=near.at[t], send_sem=n_send.at[o], recv_sem=n_recv.at[t],
            device_id=(d, lax.rem(t + o, lanes)), device_id_type=MESH,
        )

    def far_copy(o):
        return pltpu.make_async_remote_copy(
            src_ref=near, dst_ref=far.at[d], send_sem=f_send.at[o], recv_sem=f_recv.at[d],
            device_id=(lax.rem(d + o, owners), t), device_id_type=MESH,
        )

    def got(ref, sem):
        pltpu.make_async_copy(ref, ref, sem).wait()

    for o in range(1, lanes):
        near_copy(o).start()
    own = pltpu.make_async_copy(part, near.at[t], own_sem)
    own.start()
    own.wait()
    for o in range(1, lanes):
        s = lax.rem(t + o, lanes)
        got(near.at[s], n_recv.at[s])
    for o in range(1, owners):
        far_copy(o).start()
    total = jnp.sum(near[...], axis=0)
    for o in range(1, owners):
        s = lax.rem(d + o, owners)
        got(far.at[s], f_recv.at[s])
        total += jnp.sum(far[s], axis=0)
    squares = jnp.sum(total, axis=(0, 1), keepdims=True)
    scale = jnp.minimum(1.0, limit / jnp.sqrt(squares))
    factor[...] = jnp.broadcast_to(scale, factor.shape)
    for o in range(1, lanes):
        near_copy(o).wait_send()
    for o in range(1, owners):
        far_copy(o).wait_send()


def clip_factor(part, owners, lanes, limit):
    dma = pltpu.SemaphoreType.DMA
    return pl.pallas_call(
        functools.partial(norm_kernel, owners, lanes, limit),
        out_shape=jax.ShapeDtypeStruct(part.shape, part.dtype),
        in_specs=[pl.BlockSpec(memory_space=pltpu.VMEM)],
        out_specs=pl.BlockSpec(memory_space=pltpu.VMEM),
        scratch_shapes=[
            pltpu.VMEM((lanes,) + part.shape, part.dtype),
            pltpu.VMEM((owners, lanes) + part.shape, part.dtype),
            dma, dma((lanes,)), dma((lanes,)), dma((owners,)), dma((owners,)),
        ],
        compiler_params=pltpu.CompilerParams(
            collective_id=1, has_side_effects=True, vmem_limit_bytes=4 * 1024 * 1024
        ),
    )(part)


def scale_kernel(x, scale, out):
    out[0] = (x[0].astype(jnp.float32) * scale[0].astype(jnp.float32)).astype(out.dtype)


def scaled_pieces(x, scale, pieces):
    blocks, tokens, columns = x.shape
    width = columns // pieces
    if width % 128:
        whole = (x.astype(jnp.float32) * scale.astype(jnp.float32)).astype(jnp.bfloat16)
        return whole.reshape(blocks * tokens, pieces, width).transpose(1, 0, 2)
    return pl.pallas_call(
        scale_kernel,
        grid=(pieces, blocks),
        out_shape=jax.ShapeDtypeStruct((pieces, blocks * tokens, width), jnp.bfloat16),
        in_specs=[
            pl.BlockSpec((1, tokens, width), lambda p, b: (b, 0, p)),
            pl.BlockSpec((1, 1, width), lambda p, b: (b, 0, p)),
        ],
        out_specs=pl.BlockSpec((1, tokens, width), lambda p, b: (p, b, 0)),
        compiler_params=pltpu.CompilerParams(vmem_limit_bytes=8 * 1024 * 1024),
    )(x, scale)


def per_device(activations, out_grads, act_scale, grad_scale, moment, second, master):
    owners = lax.axis_size("dp")
    lanes = lax.axis_size("tensor")
    blocks, tile_tokens, weight_rows = activations.shape
    tiles = act_scale.shape[1]
    local_tokens = blocks * tile_tokens
    columns = out_grads.shape[2]
    owned = columns // owners
    entries = columns * lanes * weight_rows
    quarter = weight_rows // lanes
    spread = jnp.broadcast_to(
        act_scale.astype(jnp.float32)[:, :, None], (blocks, tiles, weight_rows // tiles)
    ).reshape(blocks, 1, weight_rows)
    acts_deq = scaled_pieces(activations, spread, lanes)
    grads_deq = scaled_pieces(out_grads, grad_scale, owners)
    piece, moved = gather_all(acts_deq, grads_deq, owners)
    total = owners * local_tokens
    moved = moved.reshape(total, owned)
    piece = piece.reshape(lanes, total, quarter)
    parts = []
    for t in range(lanes):
        parts.append(
            lax.dot_general(
                moved, piece[t], (((0,), (0,)), ((), ())), preferred_element_type=jnp.float32
            )
        )
    grad_owned = jnp.concatenate(parts, axis=1)
    part = jnp.sum((grad_owned * grad_owned).reshape(owned // 8, 8, weight_rows // 128, 128), axis=(0, 2))
    limit = clip_rms * math.sqrt(entries)
    factor = clip_factor(part, owners, lanes, limit)[0, 0]
    clipped = factor * grad_owned
    new_moment = beta_first * moment + (1.0 - beta_first) * clipped
    new_second = beta_second * second + (1.0 - beta_second) * clipped * clipped
    new_master = master - learn_rate * new_moment / (jnp.sqrt(new_second) + adam_eps)
    weights = new_master.astype(jnp.bfloat16)
    return (new_moment, new_second, new_master, weights)


def solution(mesh):
    return jax.shard_map(
        per_device,
        mesh=mesh,
        in_specs=(
            P("dp", None, None),
            P("dp", None, "tensor"),
            P("dp", None),
            P("dp", None, "tensor"),
            P(("tensor", "dp"), None),
            P(("tensor", "dp"), None),
            P(("tensor", "dp"), None),
        ),
        out_specs=(
            P(("tensor", "dp"), None),
            P(("tensor", "dp"), None),
            P(("tensor", "dp"), None),
            P(("tensor", "dp"), None),
        ),
        check_vma=False,
    )
```
